32 devices in a mesh: dp: 8 (over z, y), fsdp: 4 (over x, core).
Axes of the slice: x: 2, y: 2, z: 4, core: 2. Of those that a mesh axis runs over, the one named last changes fastest.
Arguments:
- momentum: float32 [2, 6144, 16384], P(None, 'fsdp', 'dp'), may hold values from -160 to 160, as said below
- gradient: bfloat16 [2, 6144, 16384], P(None, 'fsdp', 'dp'), may hold values from -6 to 6
- q_factor: float32 [2, 16384, 256], P(None, 'dp'), may hold values from -6 to 6
Outputs:
- new_momentum: float32 [2, 6144, 16384], P(None, 'fsdp', 'dp')
- update: bfloat16 [2, 6144, 16384], P(None, 'fsdp', 'dp')
- new_q: float32 [2, 16384, 256], P(None, 'dp')
The draws below stay inside these ranges and needn't reach their ends.
Inputs may be any that keep to these rules, and one draw needn't show every extreme that they name: `momentum`: Real-valued entries.
All inputs are finite; a program needn't handle non-finite values.
Results may differ from the reference program's by a relative error of at most 0.001.
Values sent between devices are 32-bit elements; how exact they have to be, the bound alone decides.
No kernel may reach another device: no remote copies, remote signals or barrier semaphores. Data moves between devices by JAX's collectives and lax.ppermute only.
A program may use at most 192 MiB of HBM per device.

```python
import jax
import jax.numpy as jnp
from jax import lax

M = 6144
N = 16384
R = 256
E = 2


def draw_momentum(key, part):
    random_key, row_key, col_key = jax.random.split(key, 3)
    row_place = jnp.arange(M, dtype=jnp.float32) / M - 0.5
    col_place = jnp.arange(N, dtype=jnp.float32) / N - 0.5
    random_part = jax.random.truncated_normal(random_key, -5.0, 5.0, (E, M, N), jnp.float32)
    spread = 1.15
    growth = 3.0
    row_scale = jnp.exp(row_place[None, :, None] * jnp.log(growth) + jax.random.uniform(row_key, (E, M, 1), jnp.float32, -spread, spread))
    col_scale = jnp.exp(col_place[None, None, :] * jnp.log(growth) + jax.random.uniform(col_key, (E, 1, N), jnp.float32, -spread, spread))
    return random_part * row_scale * col_scale


def steps_of(own_key, extent, cuts, low, top_value):
    loudness = 1.0
    for axis_at, parts in cuts:
        draws = jax.random.uniform(jax.random.fold_in(jax.random.fold_in(own_key, 6), axis_at), (parts,), jnp.float32, low / len(cuts), top_value / len(cuts))
        loudness = loudness * jnp.repeat(jnp.exp(draws), extent[axis_at] // parts).reshape((-1,) + (1,) * (len(extent) - 1 - axis_at))
    return loudness


def gaussian(key, shape, scale, limit, cuts=(), kind=jnp.bfloat16):
    factor_of = steps_of(key, shape, cuts, -0.22, 0.18) if cuts else 1.0
    drawn = jax.random.normal(key, shape, jnp.float32) * scale * factor_of
    return jnp.minimum(jnp.maximum(drawn, -limit), limit).astype(kind)


def setup_inputs(seed: int = 0) -> dict:
    arg_keys = jax.random.split(jax.random.key(seed), 4)
    momentum = draw_momentum(jax.random.fold_in(arg_keys[3], 71), 0)
    gradient = gaussian(arg_keys[1], (E, M, N), 1.0, 6.0, ((1, 4), (2, 8)))
    q_factor = gaussian(arg_keys[2], (E, N, R), 1.0, 6.0, ((1, 8),), jnp.float32)
    return {"momentum": momentum, "gradient": gradient, "q_factor": q_factor}


ema_decay = 0.75
epsilon = 1e-06

def one_matrix(inputs):
    moment_part, grad_part, q_part = inputs
    buffer = moment_part + grad_part.astype(jnp.float32)
    left = jnp.dot(buffer, q_part, precision=lax.Precision.HIGHEST)
    gram_matrix = jnp.dot(left.T, left, precision=lax.Precision.HIGHEST)
    lower_factor = jnp.linalg.cholesky(gram_matrix)
    orthonormal = lax.linalg.triangular_solve(lower_factor, left, left_side=False, lower=True, transpose_a=True)
    right_factor = jnp.dot(buffer.T, orthonormal, precision=lax.Precision.HIGHEST)
    new_moment = buffer - (1.0 - ema_decay) * jnp.dot(orthonormal, right_factor.T, precision=lax.Precision.HIGHEST)
    mean_square = lax.optimization_barrier(jnp.mean(right_factor * right_factor, axis=0))
    next_q = right_factor * lax.rsqrt(mean_square + epsilon)[None, :]
    direction = jnp.dot(orthonormal, next_q.T, precision=lax.Precision.HIGHEST) * jnp.sqrt(jnp.float32(M) / jnp.float32(R))
    return (new_moment, direction.astype(jnp.bfloat16), next_q)

def reference(momentum, gradient, q_factor):
    new_momentum, update, new_q = lax.map(one_matrix, (momentum, gradient, q_factor))
    return (new_momentum, update, new_q)
```

```python
import functools

import jax
import jax.numpy as jnp
from jax import lax
from jax.experimental import pallas as pl
from jax.experimental.pallas import tpu as pltpu
from jax.sharding import PartitionSpec as P

ema_decay = 0.75
epsilon = 1e-06
f32 = jnp.float32
bf16 = jnp.bfloat16
HIGHEST = lax.Precision.HIGHEST


def split(value):
    high = value.astype(bf16)
    return high, (value - high.astype(f32)).astype(bf16)


def dot(a, b):
    return lax.dot_general(a, b, (((1,), (0,)), ((), ())), preferred_element_type=f32)


def dot_exact(a, b, dims=((1,), (0,))):
    return lax.dot_general(a, b, (dims, ((), ())), precision=HIGHEST, preferred_element_type=f32)


def tile_of(size, unit, limit):
    best = size
    for tile in range(unit, min(size, limit) + 1, unit):
        if size % tile == 0:
            best = tile
    return best


def left_kernel(m_ref, g_ref, q_ref, out_ref, qh_ref, ql_ref):
    @pl.when(pl.program_id(0) == 0)
    def _():
        qh, ql = split(q_ref[0])
        qh_ref[...] = qh
        ql_ref[...] = ql

    high, low = split(m_ref[0] + g_ref[0].astype(f32))
    out_ref[...] = dot(high, qh_ref[...]) + dot(high, ql_ref[...]) + dot(low, qh_ref[...])


def left_of(e, momentum, gradient, q_factor):
    _, rows, cols = momentum.shape
    rank = q_factor.shape[2]
    tile = tile_of(rows, 16, 256)
    big = pl.BlockSpec((1, tile, cols), lambda i: (e, i, 0))
    return pl.pallas_call(
        left_kernel,
        grid=(rows // tile,),
        in_specs=[big, big, pl.BlockSpec((1, cols, rank), lambda i: (e, 0, 0))],
        out_specs=pl.BlockSpec((tile, rank), lambda i: (i, 0)),
        out_shape=jax.ShapeDtypeStruct((rows, rank), f32),
        scratch_shapes=[pltpu.VMEM((cols, rank), bf16), pltpu.VMEM((cols, rank), bf16)],
        name=f"left{e}",
    )(momentum, gradient, q_factor)


def right_kernel(m_ref, g_ref, left_ref, out_ref, gram_ref, lt_ref):
    rank = left_ref.shape[1]

    @pl.when(pl.program_id(0) == 0)
    def _():
        turned = left_ref[...].T
        high, low = split(turned)
        lt_ref[:rank] = high
        lt_ref[rank:] = low
        gram_ref[...] = dot_exact(turned, left_ref[...])

    high, low = split(m_ref[0] + g_ref[0].astype(f32))
    both = dot(lt_ref[...], high)
    out_ref[...] = both[:rank] + both[rank:] + dot(lt_ref[:rank], low)


def right_of(e, momentum, gradient, left):
    _, rows, cols = momentum.shape
    rank = left.shape[1]
    tile = tile_of(cols, 128, 512)
    big = pl.BlockSpec((1, rows, tile), lambda i: (e, 0, i))
    return pl.pallas_call(
        right_kernel,
        grid=(cols // tile,),
        in_specs=[big, big, pl.BlockSpec((rows, rank), lambda i: (0, 0))],
        out_specs=[
            pl.BlockSpec((rank, tile), lambda i: (0, i)),
            pl.BlockSpec((rank, rank), lambda i: (0, 0)),
        ],
        out_shape=[
            jax.ShapeDtypeStruct((rank, cols), f32),
            jax.ShapeDtypeStruct((rank, rank), f32),
        ],
        scratch_shapes=[pltpu.VMEM((2 * rank, rows), bf16)],
        name=f"right{e}",
    )(momentum, gradient, left)


def factor_kernel(block, gram_ref, out_ref, a_ref):
    rank = gram_ref.shape[0]
    a_ref[...] = gram_ref[...]
    row_at = lax.broadcasted_iota(jnp.int32, (rank, rank), 0)
    col_at = lax.broadcasted_iota(jnp.int32, (rank, rank), 1)
    out_ref[...] = jnp.where(row_at == col_at, 1.0, 0.0).astype(f32)
    small_row = lax.broadcasted_iota(jnp.int32, (block, 2 * block), 0)
    small_col = lax.broadcasted_iota(jnp.int32, (block, 2 * block), 1)
    unit = jnp.where(small_row[:, :block] == small_col[:, :block], 1.0, 0.0).astype(f32)

    def step(j, wide):
        pivot_row = jnp.sum(jnp.where(small_row == j, wide, 0.0), axis=0, keepdims=True)
        column = jnp.sum(jnp.where(small_col == j, wide, 0.0), axis=1, keepdims=True)
        pivot = jnp.sum(
            jnp.where(small_col[:1] == j, pivot_row, 0.0), axis=1, keepdims=True
        )
        factor = jnp.where(small_row[:, :1] > j, column, 0.0)
        return wide - factor * (pivot_row * (1.0 / pivot))

    for k in range(rank // block):
        here = slice(k * block, (k + 1) * block)
        wide = jnp.concatenate([a_ref[here, here], unit], axis=1)
        wide = lax.fori_loop(0, block, step, wide, unroll=4)
        pivots = jnp.sum(
            jnp.where(small_row[:, :block] == small_col[:, :block], wide[:, :block], 0.0),
            axis=1,
            keepdims=True,
        )
        inverse = wide[:, block:] / jnp.sqrt(pivots)
        top = dot_exact(inverse, a_ref[here, :])
        own = dot_exact(inverse, out_ref[here, :])
        out_ref[here, :] = own
        if (k + 1) * block < rank:
            later = row_at >= (k + 1) * block
            a_ref[...] -= jnp.where(later, dot_exact(top, top, ((0,), (0,))), 0.0)
            out_ref[...] -= jnp.where(later, dot_exact(top, own, ((0,), (0,))), 0.0)


def inverse_factor(e, gram):
    rank = gram.shape[0]
    return pl.pallas_call(
        functools.partial(factor_kernel, 64),
        out_shape=jax.ShapeDtypeStruct((rank, rank), f32),
        scratch_shapes=[pltpu.VMEM((rank, rank), f32)],
        name=f"factor{e}",
    )(gram)


def solve_kernel(inverse_ref, raw_ref, out_ref, squares_ref):
    value = dot_exact(inverse_ref[...], raw_ref[...])
    out_ref[...] = value
    ones = jnp.ones((8, value.shape[1]), f32)
    part = dot_exact(ones, value * value, ((1,), (1,)))

    @pl.when(pl.program_id(0) == 0)
    def _():
        squares_ref[...] = jnp.zeros_like(squares_ref)

    squares_ref[...] += part


def solved(e, inverse, raw):
    rank, cols = raw.shape
    tile = tile_of(cols, 128, 512)
    wide = pl.BlockSpec((rank, tile), lambda i: (0, i))
    return pl.pallas_call(
        solve_kernel,
        grid=(cols // tile,),
        in_specs=[pl.BlockSpec((rank, rank), lambda i: (0, 0)), wide],
        out_specs=[wide, pl.BlockSpec((8, rank), lambda i: (0, 0))],
        out_shape=[
            jax.ShapeDtypeStruct((rank, cols), f32),
            jax.ShapeDtypeStruct((8, rank), f32),
        ],
        name=f"solve{e}",
    )(inverse, raw)


def feedback_kernel(m_ref, g_ref, left_ref, inverse_ref, right_ref, *rest):
    out_ref, rh_ref = rest[-2:]

    @pl.when(pl.program_id(0) == 0)
    def _():
        rh_ref[...] = (right_ref[...] * (ema_decay - 1.0)).astype(bf16)

    ortho = dot_exact(left_ref[...], inverse_ref[...], ((1,), (1,)))
    out_ref[0] = (m_ref[0] + g_ref[0].astype(f32)) + dot(ortho.astype(bf16), rh_ref[...])


def feedback(e, momentum, gradient, left, inverse, right, before):
    matrices, rows, cols = momentum.shape
    rank = left.shape[1]
    tile = tile_of(rows, 16, 256)
    big = pl.BlockSpec((1, tile, cols), lambda i: (e, i, 0))
    extra = [] if before is None else [before]
    return pl.pallas_call(
        feedback_kernel,
        grid=(rows // tile,),
        in_specs=[
            big,
            big,
            pl.BlockSpec((tile, rank), lambda i: (i, 0)),
            pl.BlockSpec((rank, rank), lambda i: (0, 0)),
            pl.BlockSpec((rank, cols), lambda i: (0, 0)),
        ]
        + [pl.BlockSpec(memory_space=pl.ANY)] * len(extra),
        out_specs=big,
        out_shape=jax.ShapeDtypeStruct((matrices, rows, cols), f32),
        input_output_aliases={5: 0} if extra else {},
        scratch_shapes=[pltpu.VMEM((rank, cols), bf16)],
        name=f"feedback{e}",
    )(momentum, gradient, left, inverse, right, *extra)


def update_kernel(total_cols, gain, left_ref, inverse_ref, right_ref, squares_ref, *rest):
    up_ref, q_ref, qh_ref, ql_ref = rest[-4:]
    cols = right_ref.shape[1]
    step = q_ref.shape[1]
    at = pl.program_id(0)
    scale = lax.rsqrt(squares_ref[...].T[:, :1] / total_cols + epsilon)

    @pl.when(at == 0)
    def _():
        qh, ql = split(right_ref[...] * (scale * gain))
        qh_ref[...] = qh
        ql_ref[...] = ql

    own = right_ref[:, pl.ds(pl.multiple_of(at * step, 128), step)] if step < cols else right_ref[...]
    q_ref[0] = (own * scale).T
    oh, ol = split(dot_exact(left_ref[...], inverse_ref[...], ((1,), (1,))))
    total = dot(oh, qh_ref[...]) + dot(oh, ql_ref[...]) + dot(ol, qh_ref[...])
    up_ref[0] = total.astype(bf16)


def updated(e, matrices, left, inverse, right, squares, total_rows, total_cols, before):
    rows, rank = left.shape
    cols = right.shape[1]
    steps = 1
    for count in (2, 4):
        if cols % (count * 128) == 0 and rows % (count * 16) == 0:
            steps = count
    tile, step = rows // steps, cols // steps
    extra = [] if before is None else list(before)
    gain = (total_rows / rank) ** 0.5
    whole = lambda shape: pl.BlockSpec(shape, lambda i: (0, 0))
    return pl.pallas_call(
        functools.partial(update_kernel, float(total_cols), gain),
        grid=(steps,),
        in_specs=[
            pl.BlockSpec((tile, rank), lambda i: (i, 0)),
            whole((rank, rank)),
            whole((rank, cols)),
            whole((8, rank)),
        ]
        + [pl.BlockSpec(memory_space=pl.ANY)] * len(extra),
        out_specs=[
            pl.BlockSpec((1, tile, cols), lambda i: (e, i, 0)),
            pl.BlockSpec((1, step, rank), lambda i: (e, i, 0)),
        ],
        out_shape=[
            jax.ShapeDtypeStruct((matrices, rows, cols), bf16),
            jax.ShapeDtypeStruct((matrices, cols, rank), f32),
        ],
        input_output_aliases={4: 0, 5: 1} if extra else {},
        scratch_shapes=[pltpu.VMEM((rank, cols), bf16), pltpu.VMEM((rank, cols), bf16)],
        name=f"update{e}",
    )(left, inverse, right, squares, *extra)


def swap(value, axis, bit):
    return lax.ppermute(value, axis, [(i, i ^ bit) for i in range(lax.axis_size(axis))])


def exchange(value, axis, bits):
    bit = bits[0]
    if len(bits) == 1:
        return value + swap(value, axis, bit)
    half = value.shape[0] // 2
    upper = (lax.axis_index(axis) & bit) != 0
    first, second = value[:half], value[half:]
    kept = jnp.where(upper, second, first) + swap(jnp.where(upper, first, second), axis, bit)
    kept = exchange(kept, axis, bits[1:])
    other = swap(kept, axis, bit)
    return jnp.concatenate(
        [jnp.where(upper, other, kept), jnp.where(upper, kept, other)], axis=0
    )


def bits_of(axis):
    size = lax.axis_size(axis)
    return [1 << k for k in range(size.bit_length() - 1)] if size & (size - 1) == 0 else []


def summed(value, axis, parts=1):
    bits = bits_of(axis)
    pieces = value.shape[0] // parts
    if not bits or pieces % (8 * lax.axis_size(axis)):
        return lax.psum(value, axis)
    if parts == 1 or len(bits) < 3:
        return exchange(value, axis, bits)
    swapped = [bits[1], bits[0]] + bits[2:]
    return jnp.concatenate(
        [exchange(value[:pieces], axis, bits), exchange(value[pieces:], axis, swapped)], axis=0
    )


def small_sum(value, axis):
    bits = bits_of(axis)
    if not bits:
        return lax.psum(value, axis)
    for bit in bits:
        value = value + swap(value, axis, bit)
    return value


def body(momentum, gradient, q_factor):
    matrices, rows, cols = momentum.shape
    total_rows = rows * lax.axis_size("fsdp")
    total_cols = cols * lax.axis_size("dp")
    every = range(matrices)
    lefts = [summed(left_of(e, momentum, gradient, q_factor), "dp", 2) for e in every]
    pairs = [right_of(e, momentum, gradient, lefts[e]) for e in every]
    grams = [summed(pairs[e][1], "fsdp") for e in every]
    raws = [summed(pairs[e][0], "fsdp") for e in every]
    inverses = [inverse_factor(e, grams[e]) for e in every]
    rights, squares = zip(*[solved(e, inverses[e], raws[e]) for e in every])
    squares = [small_sum(s, "dp") for s in squares]
    new_momentum = None
    ups = None
    for e in every:
        new_momentum = feedback(
            e, momentum, gradient, lefts[e], inverses[e], rights[e], new_momentum
        )
    for e in every:
        ups = updated(
            e, matrices, lefts[e], inverses[e], rights[e], squares[e], total_rows, total_cols, ups
        )
    return (new_momentum, ups[0], ups[1])


def solution(mesh):
    placed = (P(None, "fsdp", "dp"), P(None, "fsdp", "dp"), P(None, "dp", None))
    return jax.shard_map(
        body,
        mesh=mesh,
        in_specs=placed,
        out_specs=(P(None, "fsdp", "dp"), P(None, "fsdp", "dp"), P(None, "dp", None)),
        check_vma=False,
    )
```
